32 devices in a mesh: grp: 2 (over y), ka: 4 (over z), orb: 2 (over x), band: 2 (over core).
Axes of the slice: x: 2, y: 2, z: 4, core: 2. Of those that a mesh axis runs over, the one named last changes fastest.
Arguments:
- eigvecs: bfloat16 [8, 2, 8192, 256], P(('grp', 'ka'), None, 'orb', 'band'), parts along dimension 0, may hold values from -0.03515625 to 0.03515625
- band_rank: int32 [8, 256], P(('grp', 'ka'), 'band'), parts along dimension 0, may hold values from 0 to 255, each once within a row
- occ_count: int32 [2], P('grp'), parts along dimension 0, may hold values from 128 to 256
- wrap_shift: int32 [2], P('grp'), parts along dimension 0, may hold values from 1 to 4095
- orbital_site: int32 [16384], P(('grp', 'orb')), parts along dimension 0, may hold values from 0 to 63
Outputs:
- wilson: float32 [8, 256, 2, 256], P(('grp', 'ka'), 'orb', None, 'band'), parts along dimension 0
The draws below stay inside these ranges and needn't reach their ends.
There are 2 independent parts, one for each index of `grp`. The reference program is written for one: setup_inputs(seed, part) draws one part's arguments, and reference() takes and returns one part's arrays. A program takes and returns all parts, laid end to end along the dimension named above; each array names one. Nothing has to cross between parts.
All inputs are finite; a program needn't handle non-finite values.
Results may differ from the reference program's by a relative error of at most 0.025.
Values may be sent and summed in bfloat16 or wider, within the bound.
A program may use at most 64 MiB of HBM per device.

```python
import math
import jax
import jax.numpy as jnp
from jax import lax

ORBS = 8192
BANDS = 256
NS_STEPS = 8
SITES = 64
KPTS = 4


def draw_eigvecs(key, part):
    entry_scale = (2.0 * ORBS) ** (-0.5)
    full_shape = (KPTS, 2, ORBS, BANDS)
    base_key = jax.random.fold_in(key, 101)
    noise_key = jax.random.fold_in(key, 202)
    mix_key = jax.random.fold_in(key, 303)
    common = jax.random.normal(base_key, (2, ORBS, BANDS), jnp.float32)
    fresh_noise = jax.random.normal(noise_key, full_shape, jnp.float32)
    mixing = jax.random.uniform(mix_key, (KPTS, 1, 1, 1), jnp.float32, 0.3, 0.55)
    values = mixing * common[None] + jnp.sqrt(1.0 - mixing * mixing) * fresh_noise
    return (jnp.clip(values, -4.4, 4.4) * entry_scale).astype(jnp.bfloat16)


def set_ends(array, key, smallest, largest):
    spot = [jax.random.randint(jax.random.fold_in(key, axis), (), 0, length) for axis, length in enumerate(array.shape)]
    main_axis = array.shape.index(max(array.shape))
    next_to = spot[:main_axis] + [(spot[main_axis] + 1) % array.shape[main_axis]] + spot[main_axis + 1:]
    return array.at[tuple(spot)].set(smallest).at[tuple(next_to)].set(largest)


def setup_inputs(seed: int = 0, part: int = 0) -> dict:
    streams_of = jax.random.split(jax.random.key(seed), 6)
    part_splits = jax.random.split(jax.random.fold_in(streams_of[5], part), 6)
    eigvecs = draw_eigvecs(jax.random.fold_in(jax.random.fold_in(streams_of[5], part), 71), part)
    band_rank = jax.vmap(lambda own: jax.random.permutation(own, BANDS))(jax.random.split(part_splits[1], KPTS)).reshape((KPTS, BANDS)).astype(jnp.int32)
    occ_count = jax.random.randint(part_splits[2], (1,), BANDS // 2, BANDS + 1).astype(jnp.int32)
    wrap_shift = jax.random.randint(part_splits[3], (1,), 1, 4096).astype(jnp.int32)
    orbital_site = set_ends(jax.random.randint(part_splits[4], (ORBS,), 0, SITES), jax.random.fold_in(part_splits[4], 1), 0, SITES - 1).astype(jnp.int32)
    return dict(eigvecs=eigvecs, band_rank=band_rank, occ_count=occ_count, wrap_shift=wrap_shift, orbital_site=orbital_site)


ns_gain = 0.7
eps_mean = 1e-06

def complex_block(matrix):
    order_size = matrix.shape[0]
    real_part = matrix[:, :order_size]
    imag_part = matrix[:, order_size:]
    upper_half = jnp.concatenate([real_part, imag_part], axis=1)
    lower_half = jnp.concatenate([-imag_part, real_part], axis=1)
    return jnp.concatenate([upper_half, lower_half], axis=0)

def complex_product(left_side, right_side):
    return jnp.dot(left_side, complex_block(right_side), precision=lax.Precision.HIGHEST, preferred_element_type=jnp.float32)

def polar_step(iterate):
    order_size = iterate.shape[1]
    rounded = iterate.astype(jnp.bfloat16)
    widened = rounded.astype(jnp.float32)
    gram_matrix = jnp.einsum('kri,krj->kij', widened, widened, precision=lax.Precision.HIGHEST)
    gram_real = gram_matrix[:, :order_size, :order_size] + gram_matrix[:, order_size:, order_size:]
    gram_imag = gram_matrix[:, :order_size, order_size:] - gram_matrix[:, order_size:, :order_size]
    upper_half = jnp.concatenate([gram_real, gram_imag], axis=2)
    lower_half = jnp.concatenate([-gram_imag, gram_real], axis=2)
    gram_block = jnp.concatenate([upper_half, lower_half], axis=1).astype(jnp.bfloat16).astype(jnp.float32)
    product = jnp.einsum('kri,kij->krj', widened, gram_block, precision=lax.Precision.HIGHEST)
    return 1.5 * iterate - 0.5 * product

def margin_pair(block_pair):
    left_block, right_block = block_pair
    stacked = jnp.concatenate([left_block[0], left_block[1]], axis=0)
    real_side = jnp.concatenate([right_block[0], right_block[1]], axis=0)
    imag_side = jnp.concatenate([right_block[1], -right_block[0]], axis=0)
    paired = jnp.concatenate([real_side, imag_side], axis=1)
    return jnp.dot(stacked.T, paired, preferred_element_type=jnp.float32)

def reference(eigvecs, band_rank, occ_count, wrap_shift, orbital_site):
    occupied = band_rank < occ_count[0]
    masked = jnp.where(occupied[:, None, None, :], eigvecs, jnp.zeros((), jnp.bfloat16))
    phase_angle = (wrap_shift[0] * orbital_site % SITES).astype(jnp.float32) * (2.0 * math.pi / SITES)
    cosine = jnp.cos(phase_angle)[:, None]
    sine_factor = jnp.sin(phase_angle)[:, None]
    first_real = masked[0, 0].astype(jnp.float32)
    first_imag = masked[0, 1].astype(jnp.float32)
    wrapped = jnp.stack([cosine * first_real + sine_factor * first_imag, cosine * first_imag - sine_factor * first_real]).astype(jnp.bfloat16)
    right_blocks = jnp.concatenate([masked[1:], wrapped[None]], axis=0)
    margins = lax.map(margin_pair, (masked, right_blocks))
    occupied_total = occ_count[0].astype(jnp.float32)
    squares = lax.optimization_barrier(jnp.sum(margins * margins, axis=(1, 2)))
    iterate = margins * (ns_gain * lax.rsqrt(squares / occupied_total + eps_mean))[:, None, None]
    for sweep_index in range(NS_STEPS):
        iterate = polar_step(iterate)
    identity = jnp.concatenate([jnp.eye(BANDS, dtype=jnp.float32), jnp.zeros((BANDS, BANDS), jnp.float32)], axis=1)

    def link(running, factor):
        following = complex_product(running, factor)
        return (following, following)
    final_loop, prefix = lax.scan(link, identity, iterate)
    return prefix.reshape(KPTS, BANDS, 2, BANDS) * math.sqrt(BANDS)
```

```python
import functools
import math

import jax
import jax.numpy as jnp
from jax import lax
from jax.experimental import pallas as pl
from jax.experimental.pallas import tpu as pltpu
from jax.sharding import PartitionSpec as P

NS_STEPS = 8
SITES = 64
CHUNKS = 8

ns_gain = 0.7
eps_mean = 1e-06

MESH = pl.DeviceIdType.MESH
BF16 = jnp.bfloat16
F32 = jnp.float32


def levels_of(count):
    return max(1, (count - 1).bit_length())


def remote(src, dst, send_sem, recv_sem, device):
    return pltpu.make_async_remote_copy(
        src_ref=src,
        dst_ref=dst,
        send_sem=send_sem,
        recv_sem=recv_sem,
        device_id=device,
        device_id_type=MESH,
    )


def across(left, right, contract):
    return lax.dot_general(left, right, (contract, ((), ())), preferred_element_type=F32)


def column_of(row, width):
    return jnp.transpose(jnp.broadcast_to(row, (width, row.shape[1])))


def polar_step(iterate):
    half = iterate.shape[1] // 2
    rounded = iterate.astype(BF16)
    real, imag = rounded[:, :half], rounded[:, half:]
    tall = jnp.concatenate(
        [rounded, jnp.concatenate([imag, -real], axis=1)], axis=0
    )
    gram = across(tall, rounded, ((1,), (1,))).astype(BF16)
    rows = iterate.shape[0]
    wide = jnp.concatenate([gram[:rows], gram[rows:]], axis=1)
    block = jnp.concatenate(
        [rounded, jnp.concatenate([-imag, real], axis=1)], axis=0
    )
    product = across(wide, block, ((1,), (0,)))
    return 1.5 * iterate - 0.5 * product


def merge(pieces, factor):
    cols = factor.shape[1] // 2
    left = jnp.concatenate(
        [piece[:, :cols] for piece in pieces] + [piece[:, cols:] for piece in pieces], axis=1
    )
    lower = jnp.concatenate([-factor[:, cols:], factor[:, :cols]], axis=1)
    return across(left, jnp.concatenate([factor, lower], axis=0), ((1,), (0,)))


def kernel(
    nka, norb, nband,
    eig, rank, occ, shift, site,
    out,
    lefts, rights, cosine, sine, angle_cos, angle_sin,
    rank_band, rank_next, acc, part_out, part_in, whole, cur, pfx, got,
    sem_own, sem_left, sem_rank, sem_next, sem_right, sem_orb, sem_sum, sem_pre, sem_fwd,
):
    ka, orb, band = lax.axis_index("ka"), lax.axis_index("orb"), lax.axis_index("band")
    rows, cols = eig.shape[1], eig.shape[2]
    bands = nband * cols
    step = rows // CHUNKS
    before = lax.rem(ka + nka - 1, nka)

    barrier = pltpu.get_barrier_semaphore()
    greeted = 0
    for axis, mine, count in (("ka", ka, nka), ("band", band, nband), ("orb", orb, norb)):
        for d in range(1, count):
            pl.semaphore_signal(
                barrier, inc=1, device_id={axis: lax.rem(mine + d, count)}, device_id_type=MESH
            )
            greeted += 1
    pl.semaphore_wait(barrier, greeted)

    def chunk(c):
        return pl.ds(c * step, step)

    sends = []
    for c in range(CHUNKS):
        copy = remote(
            eig.at[:, chunk(c)], rights.at[:, chunk(c)],
            sem_right.at[0, c], sem_right.at[1, c], {"ka": before},
        )
        copy.start()
        sends.append(copy)
    next_rank = remote(rank, rank_next, sem_next.at[0], sem_next.at[1], {"ka": before})
    next_rank.start()
    own = pltpu.make_async_copy(eig, lefts.at[:, band], sem_own)
    own.start()
    band_sends = []
    for d in range(1, nband):
        to = {"band": lax.rem(band + d, nband)}
        copy = remote(eig, lefts.at[:, band], sem_left.at[0, d], sem_left.at[1, d], to)
        copy.start()
        band_sends.append(copy)
        copy = remote(rank, rank_band.at[band], sem_rank.at[0, d], sem_rank.at[1, d], to)
        copy.start()
        band_sends.append(copy)

    at_end = ka == nka - 1
    lanes = site.shape[1]
    angle = ((shift[0] * site[...]) & (SITES - 1)).astype(F32) * (2.0 * math.pi / SITES)
    angle_cos[...] = jnp.where(at_end, jnp.cos(angle), 1.0)
    angle_sin[...] = jnp.where(at_end, jnp.sin(angle), 0.0)

    @pl.loop(0, site.shape[0])
    def _(i):
        place = pl.ds(pl.multiple_of(i * lanes, lanes), lanes)
        cosine[place, :] = column_of(angle_cos[pl.ds(i, 1), :], cols)
        sine[place, :] = column_of(angle_sin[pl.ds(i, 1), :], cols)

    rank_band[band] = rank[...]
    own.wait()
    for d in range(1, nband):
        came = lax.rem(band + nband - d, nband)
        to = {"band": lax.rem(band + d, nband)}
        remote(eig, lefts.at[:, came], sem_left.at[0, d], sem_left.at[1, d], to).wait_recv()
        remote(rank, rank_band.at[came], sem_rank.at[0, d], sem_rank.at[1, d], to).wait_recv()
    next_rank.wait_recv()

    count = occ[0]
    row_mask = jnp.concatenate(
        [column_of((rank_band[j] < count).astype(F32), cols) for j in range(nband)], axis=0
    )
    row_mask = jnp.concatenate([row_mask, row_mask], axis=1)
    col_mask = (rank_next[...] < count).astype(F32)
    col_mask = jnp.concatenate([col_mask, col_mask], axis=1)
    mask = row_mask * col_mask > 0.5

    for c in range(CHUNKS):
        sends[c].wait_recv()
        real, imag = rights[0, chunk(c), :].astype(F32), rights[1, chunk(c), :].astype(F32)
        turn, lift = cosine[chunk(c), :], sine[chunk(c), :]
        new_real = (turn * real + lift * imag).astype(BF16)
        new_imag = (turn * imag - lift * real).astype(BF16)
        paired = jnp.concatenate(
            [
                jnp.concatenate([new_real, new_imag], axis=1),
                jnp.concatenate([new_imag, -new_real], axis=1),
            ],
            axis=0,
        )
        stacked = jnp.concatenate(
            [
                jnp.concatenate([lefts[p, j, chunk(c), :] for j in range(nband)], axis=1)
                for p in range(2)
            ],
            axis=0,
        )
        term = across(stacked, paired, ((0,), (0,)))
        if c == 0:
            acc[...] = term
        elif c < CHUNKS - 1:
            acc[...] += term
        else:
            part_out[...] = jnp.where(mask, acc[...] + term, 0.0).astype(BF16)

    part_sends = []
    for d in range(1, norb):
        copy = remote(
            part_out, part_in.at[d], sem_orb.at[0, d], sem_orb.at[1, d],
            {"orb": lax.rem(orb + d, norb)},
        )
        copy.start()
        part_sends.append(copy)
    total = part_out[...].astype(F32)
    for d in range(1, norb):
        part_sends[d - 1].wait_recv()
        total += part_in[d].astype(F32)
    whole[band] = total

    sum_sends = []
    for d in range(1, nband):
        copy = remote(
            whole.at[band], whole.at[band], sem_sum.at[0, d], sem_sum.at[1, d],
            {"band": lax.rem(band + d, nband)},
        )
        copy.start()
        sum_sends.append(copy)
    for d in range(1, nband):
        came = lax.rem(band + nband - d, nband)
        remote(
            whole.at[came], whole.at[came], sem_sum.at[0, d], sem_sum.at[1, d],
            {"band": lax.rem(band + d, nband)},
        ).wait_recv()
    margins = jnp.concatenate(
        [whole[j][:, :cols] for j in range(nband)] + [whole[j][:, cols:] for j in range(nband)],
        axis=1,
    )
    squares = jnp.sum(margins * margins, keepdims=True)
    iterate = margins * (ns_gain * lax.rsqrt(squares / count.astype(F32) + eps_mean))
    for _ in range(NS_STEPS):
        iterate = polar_step(iterate)

    def columns(j):
        at = [iterate[:, p * bands + j * cols : p * bands + (j + 1) * cols] for p in range(2)]
        return jnp.concatenate(at, axis=1)

    mine = columns(0)
    for j in range(1, nband):
        mine = jnp.where(band == j, columns(j), mine)
    cur[...] = mine.astype(BF16)
    share = bands // norb
    my_rows = pl.ds(pl.multiple_of(orb * share, share), share)
    scale = math.sqrt(bands)

    @pl.when(ka == 0)
    def _():
        acc[...] = mine
        out[...] = acc[my_rows, :] * scale
        pfx[...] = cur[my_rows, :]

    for level in range(levels_of(nka) if nka > 1 else 0):
        half = 1 << level
        first = ka < 2 * half
        for is_first in (True, False):
            if not is_first and 2 * half >= nka:
                continue
            height = share if is_first else bands
            source = pfx if is_first else cur
            here = first if is_first else jnp.logical_not(first)
            sending = jnp.logical_and(here, lax.rem(ka, 2 * half) == half - 1)
            taking = jnp.logical_and(here, lax.rem(ka // half, 2) == 1)

            def push(t, level=level, height=height, source=source):
                return remote(
                    source, got.at[level, band, pl.ds(0, height)],
                    sem_pre.at[0, level, t], sem_pre.at[1, level, 0],
                    {"ka": lax.rem(ka + t, nka)},
                )

            def pass_on(d, level=level, height=height):
                block = got.at[level, band, pl.ds(0, height)]
                return remote(
                    block, block, sem_fwd.at[0, level, d], sem_fwd.at[1, level, d],
                    {"band": lax.rem(band + d, nband)},
                )

            for t in range(half, 0, -1):
                @pl.when(jnp.logical_and(sending, ka + t < nka))
                def _(t=t, push=push):
                    push(t).start()

            for t in range(half, 0, -1):
                @pl.when(jnp.logical_and(sending, ka + t < nka))
                def _(t=t, push=push):
                    push(t).wait_send()

            @pl.when(taking)
            def _(level=level, height=height, is_first=is_first, push=push, pass_on=pass_on):
                push(1).wait_recv()
                for d in range(1, nband):
                    pass_on(d).start()
                for d in range(1, nband):
                    came = lax.rem(band + nband - d, nband)
                    block = got.at[level, came, pl.ds(0, height)]
                    remote(
                        block, block, sem_fwd.at[0, level, d], sem_fwd.at[1, level, d],
                        {"band": lax.rem(band + d, nband)},
                    ).wait_recv()
                pieces = [got[level, j, :height, :] for j in range(nband)]
                joined = merge(pieces, cur[...])
                if is_first:
                    out[...] = joined * scale
                    pfx[...] = joined.astype(BF16)
                else:
                    cur[...] = joined.astype(BF16)
                for d in range(1, nband):
                    pass_on(d).wait_send()

    for copy in sends + band_sends + part_sends + sum_sends + [next_rank]:
        copy.wait_send()


def solution(mesh):
    nka, norb, nband = mesh.shape["ka"], mesh.shape["orb"], mesh.shape["band"]
    depth = levels_of(nka)

    def body(eigvecs, band_rank, occ_count, wrap_shift, orbital_site):
        rows, cols = eigvecs.shape[2], eigvecs.shape[3]
        bands = cols * nband
        share = bands // norb
        vmem = pl.BlockSpec(memory_space=pltpu.VMEM)
        smem = pl.BlockSpec(memory_space=pltpu.SMEM)
        dma = pltpu.SemaphoreType.DMA
        result = pl.pallas_call(
            functools.partial(kernel, nka, norb, nband),
            out_shape=jax.ShapeDtypeStruct((share, 2 * cols), F32),
            in_specs=[pl.BlockSpec(memory_space=pl.ANY), vmem, smem, smem, vmem],
            out_specs=vmem,
            scratch_shapes=[
                pltpu.VMEM((2, nband, rows, cols), BF16),
                pltpu.VMEM((2, rows, cols), BF16),
                pltpu.VMEM((rows, cols), F32),
                pltpu.VMEM((rows, cols), F32),
                pltpu.VMEM((rows // 128, 128), F32),
                pltpu.VMEM((rows // 128, 128), F32),
                pltpu.VMEM((nband, 1, cols), jnp.int32),
                pltpu.VMEM((1, cols), jnp.int32),
                pltpu.VMEM((bands, 2 * cols), F32),
                pltpu.VMEM((bands, 2 * cols), BF16),
                pltpu.VMEM((norb, bands, 2 * cols), BF16),
                pltpu.VMEM((nband, bands, 2 * cols), F32),
                pltpu.VMEM((bands, 2 * cols), BF16),
                pltpu.VMEM((share, 2 * cols), BF16),
                pltpu.VMEM((depth, nband, bands, 2 * cols), BF16),
                dma,
                dma((2, nband)),
                dma((2, nband)),
                dma((2,)),
                dma((2, CHUNKS)),
                dma((2, norb)),
                dma((2, nband)),
                dma((2, depth, max(2, 1 << (depth - 1)) + 1)),
                dma((2, depth, nband)),
            ],
            compiler_params=pltpu.CompilerParams(
                collective_id=0, has_side_effects=True, vmem_limit_bytes=48 * 1024 * 1024
            ),
            name="wilson",
        )(
            eigvecs.reshape(2, rows, cols), band_rank, occ_count, wrap_shift,
            orbital_site.reshape(rows // 128, 128),
        )
        return result.reshape(1, share, 2, cols)

    return jax.shard_map(
        body,
        mesh=mesh,
        in_specs=(
            P(("grp", "ka"), None, "orb", "band"),
            P(("grp", "ka"), "band"),
            P("grp"),
            P("grp"),
            P(("grp", "orb")),
        ),
        out_specs=P(("grp", "ka"), "orb", None, "band"),
        check_vma=False,
    )
```

```python
import functools
import math

import jax
import jax.numpy as jnp
from jax import lax
from jax.experimental import pallas as pl
from jax.experimental.pallas import tpu as pltpu
from jax.sharding import PartitionSpec as P

NS_STEPS = 8
SITES = 64
CHUNKS = 16

ns_gain = 0.7
eps_mean = 1e-06

MESH = pl.DeviceIdType.MESH
BF16 = jnp.bfloat16
F32 = jnp.float32


def levels_of(count):
    return max(1, (count - 1).bit_length())


def remote(src, dst, send_sem, recv_sem, device):
    return pltpu.make_async_remote_copy(
        src_ref=src,
        dst_ref=dst,
        send_sem=send_sem,
        recv_sem=recv_sem,
        device_id=device,
        device_id_type=MESH,
    )


def across(left, right, contract):
    return lax.dot_general(left, right, (contract, ((), ())), preferred_element_type=F32)


def column_of(row, width):
    return jnp.transpose(jnp.broadcast_to(row, (width, row.shape[1])))


def polar_step(iterate):
    half = iterate.shape[1] // 2
    rounded = iterate.astype(BF16)
    real, imag = rounded[:, :half], rounded[:, half:]
    tall = jnp.concatenate(
        [rounded, jnp.concatenate([imag, -real], axis=1)], axis=0
    )
    gram = across(tall, rounded, ((1,), (1,))).astype(BF16)
    rows = iterate.shape[0]
    wide = jnp.concatenate([gram[:rows], gram[rows:]], axis=1)
    block = jnp.concatenate(
        [rounded, jnp.concatenate([-imag, real], axis=1)], axis=0
    )
    product = across(wide, block, ((1,), (0,)))
    return 1.5 * iterate - 0.5 * product


def merge(pieces, factor):
    cols = factor.shape[1] // 2
    left = jnp.concatenate(
        [piece[:, :cols] for piece in pieces] + [piece[:, cols:] for piece in pieces], axis=1
    )
    lower = jnp.concatenate([-factor[:, cols:], factor[:, :cols]], axis=1)
    return across(left, jnp.concatenate([factor, lower], axis=0), ((1,), (0,)))


def kernel(
    nka, norb, nband,
    eig, rank, occ_at, shift_at, site_at,
    out,
    lefts, rights, cosine, sine, angle_cos, angle_sin,
    occ, shift, site, rank_band, rank_next, acc, part_out, part_in, whole, cur, pfx, got,
    sem_own, sem_arg, sem_left, sem_rank, sem_next, sem_right, sem_orb, sem_sum, sem_pre, sem_fwd,
):
    ka, orb, band = lax.axis_index("ka"), lax.axis_index("orb"), lax.axis_index("band")
    rows, cols = eig.shape[1], eig.shape[2]
    bands = nband * cols
    step = rows // CHUNKS
    before = lax.rem(ka + nka - 1, nka)

    barrier = pltpu.get_barrier_semaphore()
    greeted = 0
    for axis, mine, count in (("ka", ka, nka), ("band", band, nband), ("orb", orb, norb)):
        for d in range(1, count):
            pl.semaphore_signal(
                barrier, inc=1, device_id={axis: lax.rem(mine + d, count)}, device_id_type=MESH
            )
            greeted += 1
    pl.semaphore_wait(barrier, greeted)

    def chunk(c):
        return pl.ds(c * step, step)

    next_rank = remote(rank, rank_next, sem_next.at[0], sem_next.at[1], {"ka": before})
    next_rank.start()
    sends = []
    for c in range(CHUNKS):
        copy = remote(
            eig.at[:, chunk(c)], rights.at[:, chunk(c)],
            sem_right.at[0, c], sem_right.at[1, c], {"ka": before},
        )
        copy.start()
        sends.append(copy)
    arguments = [
        pltpu.make_async_copy(src, dst, sem_arg.at[i])
        for i, (src, dst) in enumerate(
            ((occ_at, occ), (shift_at, shift), (site_at, site), (rank, rank_band.at[band]))
        )
    ]
    for copy in arguments:
        copy.start()
    own = pltpu.make_async_copy(eig, lefts.at[:, band], sem_own)
    own.start()
    band_sends = []
    for d in range(1, nband):
        to = {"band": lax.rem(band + d, nband)}
        copy = remote(eig, lefts.at[:, band], sem_left.at[0, d], sem_left.at[1, d], to)
        copy.start()
        band_sends.append(copy)
        copy = remote(rank, rank_band.at[band], sem_rank.at[0, d], sem_rank.at[1, d], to)
        copy.start()
        band_sends.append(copy)

    for copy in arguments:
        copy.wait()

    at_end = ka == nka - 1
    lanes = site.shape[1]
    angle = ((shift[0] * site[...]) & (SITES - 1)).astype(F32) * (2.0 * math.pi / SITES)
    angle_cos[...] = jnp.where(at_end, jnp.cos(angle), 1.0)
    angle_sin[...] = jnp.where(at_end, jnp.sin(angle), 0.0)

    @pl.loop(0, site.shape[0])
    def _(i):
        place = pl.ds(pl.multiple_of(i * lanes, lanes), lanes)
        cosine[place, :] = column_of(angle_cos[pl.ds(i, 1), :], cols)
        sine[place, :] = column_of(angle_sin[pl.ds(i, 1), :], cols)

    own.wait()
    for d in range(1, nband):
        came = lax.rem(band + nband - d, nband)
        to = {"band": lax.rem(band + d, nband)}
        remote(eig, lefts.at[:, came], sem_left.at[0, d], sem_left.at[1, d], to).wait_recv()
        remote(rank, rank_band.at[came], sem_rank.at[0, d], sem_rank.at[1, d], to).wait_recv()
    next_rank.wait_recv()

    count = occ[0]
    row_mask = jnp.concatenate(
        [column_of((rank_band[j] < count).astype(F32), cols) for j in range(nband)], axis=0
    )
    row_mask = jnp.concatenate([row_mask, row_mask], axis=1)
    col_mask = (rank_next[...] < count).astype(F32)
    col_mask = jnp.concatenate([col_mask, col_mask], axis=1)
    mask = row_mask * col_mask > 0.5

    for c in range(CHUNKS):
        sends[c].wait_recv()
        real, imag = rights[0, chunk(c), :].astype(F32), rights[1, chunk(c), :].astype(F32)
        turn, lift = cosine[chunk(c), :], sine[chunk(c), :]
        new_real = (turn * real + lift * imag).astype(BF16)
        new_imag = (turn * imag - lift * real).astype(BF16)
        paired = jnp.concatenate(
            [
                jnp.concatenate([new_real, new_imag], axis=1),
                jnp.concatenate([new_imag, -new_real], axis=1),
            ],
            axis=0,
        )
        stacked = jnp.concatenate(
            [
                jnp.concatenate([lefts[p, j, chunk(c), :] for j in range(nband)], axis=1)
                for p in range(2)
            ],
            axis=0,
        )
        term = across(stacked, paired, ((0,), (0,)))
        if c == 0:
            acc[...] = term
        elif c < CHUNKS - 1:
            acc[...] += term
        else:
            part_out[...] = jnp.where(mask, acc[...] + term, 0.0).astype(BF16)

    part_sends = []
    for d in range(1, norb):
        copy = remote(
            part_out, part_in.at[d], sem_orb.at[0, d], sem_orb.at[1, d],
            {"orb": lax.rem(orb + d, norb)},
        )
        copy.start()
        part_sends.append(copy)
    total = part_out[...].astype(F32)
    for d in range(1, norb):
        part_sends[d - 1].wait_recv()
        total += part_in[d].astype(F32)
    whole[band] = total

    sum_sends = []
    for d in range(1, nband):
        copy = remote(
            whole.at[band], whole.at[band], sem_sum.at[0, d], sem_sum.at[1, d],
            {"band": lax.rem(band + d, nband)},
        )
        copy.start()
        sum_sends.append(copy)
    for d in range(1, nband):
        came = lax.rem(band + nband - d, nband)
        remote(
            whole.at[came], whole.at[came], sem_sum.at[0, d], sem_sum.at[1, d],
            {"band": lax.rem(band + d, nband)},
        ).wait_recv()
    margins = jnp.concatenate(
        [whole[j][:, :cols] for j in range(nband)] + [whole[j][:, cols:] for j in range(nband)],
        axis=1,
    )
    squares = jnp.sum(margins * margins, keepdims=True)
    iterate = margins * (ns_gain * lax.rsqrt(squares / count.astype(F32) + eps_mean))
    for _ in range(NS_STEPS):
        iterate = polar_step(iterate)

    def columns(j):
        at = [iterate[:, p * bands + j * cols : p * bands + (j + 1) * cols] for p in range(2)]
        return jnp.concatenate(at, axis=1)

    mine = columns(0)
    for j in range(1, nband):
        mine = jnp.where(band == j, columns(j), mine)
    cur[...] = mine.astype(BF16)
    share = bands // norb
    my_rows = pl.ds(pl.multiple_of(orb * share, share), share)
    scale = math.sqrt(bands)

    @pl.when(ka == 0)
    def _():
        acc[...] = mine
        out[...] = acc[my_rows, :] * scale
        pfx[...] = cur[my_rows, :]

    for level in range(levels_of(nka) if nka > 1 else 0):
        half = 1 << level
        first = ka < 2 * half
        for is_first in (True, False):
            if not is_first and 2 * half >= nka:
                continue
            height = share if is_first else bands
            source = pfx if is_first else cur
            here = first if is_first else jnp.logical_not(first)
            sending = jnp.logical_and(here, lax.rem(ka, 2 * half) == half - 1)
            taking = jnp.logical_and(here, lax.rem(ka // half, 2) == 1)

            def push(t, level=level, height=height, source=source):
                return remote(
                    source, got.at[level, band, pl.ds(0, height)],
                    sem_pre.at[0, level, t], sem_pre.at[1, level, 0],
                    {"ka": lax.rem(ka + t, nka)},
                )

            def pass_on(d, level=level, height=height):
                block = got.at[level, band, pl.ds(0, height)]
                return remote(
                    block, block, sem_fwd.at[0, level, d], sem_fwd.at[1, level, d],
                    {"band": lax.rem(band + d, nband)},
                )

            for t in range(half, 0, -1):
                @pl.when(jnp.logical_and(sending, ka + t < nka))
                def _(t=t, push=push):
                    push(t).start()

            for t in range(half, 0, -1):
                @pl.when(jnp.logical_and(sending, ka + t < nka))
                def _(t=t, push=push):
                    push(t).wait_send()

            @pl.when(taking)
            def _(level=level, height=height, is_first=is_first, push=push, pass_on=pass_on):
                push(1).wait_recv()
                for d in range(1, nband):
                    pass_on(d).start()
                for d in range(1, nband):
                    came = lax.rem(band + nband - d, nband)
                    block = got.at[level, came, pl.ds(0, height)]
                    remote(
                        block, block, sem_fwd.at[0, level, d], sem_fwd.at[1, level, d],
                        {"band": lax.rem(band + d, nband)},
                    ).wait_recv()
                pieces = [got[level, j, :height, :] for j in range(nband)]
                joined = merge(pieces, cur[...])
                if is_first:
                    out[...] = joined * scale
                    pfx[...] = joined.astype(BF16)
                else:
                    cur[...] = joined.astype(BF16)
                for d in range(1, nband):
                    pass_on(d).wait_send()

    for copy in sends + band_sends + part_sends + sum_sends + [next_rank]:
        copy.wait_send()


def solution(mesh):
    nka, norb, nband = mesh.shape["ka"], mesh.shape["orb"], mesh.shape["band"]
    depth = levels_of(nka)

    def body(eigvecs, band_rank, occ_count, wrap_shift, orbital_site):
        rows, cols = eigvecs.shape[2], eigvecs.shape[3]
        bands = cols * nband
        share = bands // norb
        hbm = pl.BlockSpec(memory_space=pltpu.HBM)
        dma = pltpu.SemaphoreType.DMA
        result = pl.pallas_call(
            functools.partial(kernel, nka, norb, nband),
            out_shape=jax.ShapeDtypeStruct((share, 2 * cols), F32),
            in_specs=[hbm] * 5,
            out_specs=pl.BlockSpec(memory_space=pltpu.VMEM),
            scratch_shapes=[
                pltpu.VMEM((2, nband, rows, cols), BF16),
                pltpu.VMEM((2, rows, cols), BF16),
                pltpu.VMEM((rows, cols), F32),
                pltpu.VMEM((rows, cols), F32),
                pltpu.VMEM((rows // 128, 128), F32),
                pltpu.VMEM((rows // 128, 128), F32),
                pltpu.SMEM((1,), jnp.int32),
                pltpu.SMEM((1,), jnp.int32),
                pltpu.VMEM((rows // 128, 128), jnp.int32),
                pltpu.VMEM((nband, 1, cols), jnp.int32),
                pltpu.VMEM((1, cols), jnp.int32),
                pltpu.VMEM((bands, 2 * cols), F32),
                pltpu.VMEM((bands, 2 * cols), BF16),
                pltpu.VMEM((norb, bands, 2 * cols), BF16),
                pltpu.VMEM((nband, bands, 2 * cols), F32),
                pltpu.VMEM((bands, 2 * cols), BF16),
                pltpu.VMEM((share, 2 * cols), BF16),
                pltpu.VMEM((depth, nband, bands, 2 * cols), BF16),
                dma,
                dma((4,)),
                dma((2, nband)),
                dma((2, nband)),
                dma((2,)),
                dma((2, CHUNKS)),
                dma((2, norb)),
                dma((2, nband)),
                dma((2, depth, max(2, 1 << (depth - 1)) + 1)),
                dma((2, depth, nband)),
            ],
            compiler_params=pltpu.CompilerParams(
                collective_id=0, has_side_effects=True, vmem_limit_bytes=67043328
            ),
            name="wilson",
        )(
            eigvecs.reshape(2, rows, cols), band_rank, occ_count, wrap_shift,
            orbital_site.reshape(rows // 128, 128),
        )
        return result.reshape(1, share, 2, cols)

    return jax.shard_map(
        body,
        mesh=mesh,
        in_specs=(
            P(("grp", "ka"), None, "orb", "band"),
            P(("grp", "ka"), "band"),
            P("grp"),
            P("grp"),
            P(("grp", "orb")),
        ),
        out_specs=P(("grp", "ka"), "orb", None, "band"),
        check_vma=False,
    )
```

```python
import functools
import math

import jax
import jax.numpy as jnp
from jax import lax
from jax.experimental import pallas as pl
from jax.experimental.pallas import tpu as pltpu
from jax.sharding import PartitionSpec as P

NS_STEPS = 8
SITES = 64
CHUNKS = 16

ns_gain = 0.7
eps_mean = 1e-06

MESH = pl.DeviceIdType.MESH
BF16 = jnp.bfloat16
F32 = jnp.float32


def levels_of(count):
    return max(1, (count - 1).bit_length())


def remote(src, dst, send_sem, recv_sem, device):
    return pltpu.make_async_remote_copy(
        src_ref=src,
        dst_ref=dst,
        send_sem=send_sem,
        recv_sem=recv_sem,
        device_id=device,
        device_id_type=MESH,
    )


def across(left, right, contract):
    return lax.dot_general(left, right, (contract, ((), ())), preferred_element_type=F32)


def column_of(row, width):
    return jnp.transpose(jnp.broadcast_to(row, (width, row.shape[1])))


def polar_step(iterate):
    half = iterate.shape[1] // 2
    rounded = iterate.astype(BF16)
    real, imag = rounded[:, :half], rounded[:, half:]
    tall = jnp.concatenate(
        [rounded, jnp.concatenate([imag, -real], axis=1)], axis=0
    )
    gram = across(tall, rounded, ((1,), (1,))).astype(BF16)
    rows = iterate.shape[0]
    wide = jnp.concatenate([gram[:rows], gram[rows:]], axis=1)
    block = jnp.concatenate(
        [rounded, jnp.concatenate([-imag, real], axis=1)], axis=0
    )
    product = across(wide, block, ((1,), (0,)))
    return 1.5 * iterate - 0.5 * product


def merge(pieces, factor):
    cols = factor.shape[1] // 2
    left = jnp.concatenate(
        [piece[:, :cols] for piece in pieces] + [piece[:, cols:] for piece in pieces], axis=1
    )
    lower = jnp.concatenate([-factor[:, cols:], factor[:, :cols]], axis=1)
    return across(left, jnp.concatenate([factor, lower], axis=0), ((1,), (0,)))


def kernel(
    nka, norb, nband,
    eig, rank, occ_at, shift_at, site_at,
    out,
    lefts, rights, cosine, sine, angle_cos, angle_sin,
    occ, shift, site, rank_band, rank_next, acc, parts, cur, pfx, got,
    sem_own, sem_arg, sem_left, sem_rank, sem_next, sem_right, sem_orb, sem_sum, sem_pre, sem_fwd,
):
    ka, orb, band = lax.axis_index("ka"), lax.axis_index("orb"), lax.axis_index("band")
    rows, cols = eig.shape[1], eig.shape[2]
    bands = nband * cols
    step = rows // CHUNKS
    before = lax.rem(ka + nka - 1, nka)

    barrier = pltpu.get_barrier_semaphore()
    greeted = 0
    for axis, mine, count in (("ka", ka, nka), ("band", band, nband), ("orb", orb, norb)):
        for d in range(1, count):
            pl.semaphore_signal(
                barrier, inc=1, device_id={axis: lax.rem(mine + d, count)}, device_id_type=MESH
            )
            greeted += 1
    pl.semaphore_wait(barrier, greeted)

    def chunk(c):
        return pl.ds(c * step, step)

    next_rank = remote(rank, rank_next, sem_next.at[0], sem_next.at[1], {"ka": before})
    next_rank.start()
    sends = []
    for c in range(CHUNKS):
        copy = remote(
            eig.at[:, chunk(c)], rights.at[:, chunk(c)],
            sem_right.at[0, c], sem_right.at[1, c], {"ka": before},
        )
        copy.start()
        sends.append(copy)
    arguments = [
        pltpu.make_async_copy(src, dst, sem_arg.at[i])
        for i, (src, dst) in enumerate(
            ((occ_at, occ), (shift_at, shift), (site_at, site), (rank, rank_band.at[band]))
        )
    ]
    for copy in arguments:
        copy.start()
    own = pltpu.make_async_copy(eig, lefts.at[:, band], sem_own)
    own.start()
    band_sends = []
    for d in range(1, nband):
        to = {"band": lax.rem(band + d, nband)}
        copy = remote(eig, lefts.at[:, band], sem_left.at[0, d], sem_left.at[1, d], to)
        copy.start()
        band_sends.append(copy)
        copy = remote(rank, rank_band.at[band], sem_rank.at[0, d], sem_rank.at[1, d], to)
        copy.start()
        band_sends.append(copy)

    for copy in arguments:
        copy.wait()

    at_end = ka == nka - 1
    lanes = site.shape[1]
    angle = ((shift[0] * site[...]) & (SITES - 1)).astype(F32) * (2.0 * math.pi / SITES)
    angle_cos[...] = jnp.where(at_end, jnp.cos(angle), 1.0)
    angle_sin[...] = jnp.where(at_end, jnp.sin(angle), 0.0)

    @pl.loop(0, site.shape[0])
    def _(i):
        place = pl.ds(pl.multiple_of(i * lanes, lanes), lanes)
        cosine[place, :] = column_of(angle_cos[pl.ds(i, 1), :], cols)
        sine[place, :] = column_of(angle_sin[pl.ds(i, 1), :], cols)

    own.wait()
    for d in range(1, nband):
        came = lax.rem(band + nband - d, nband)
        to = {"band": lax.rem(band + d, nband)}
        remote(eig, lefts.at[:, came], sem_left.at[0, d], sem_left.at[1, d], to).wait_recv()
        remote(rank, rank_band.at[came], sem_rank.at[0, d], sem_rank.at[1, d], to).wait_recv()
    next_rank.wait_recv()

    count = occ[0]
    row_mask = jnp.concatenate(
        [column_of((rank_band[j] < count).astype(F32), cols) for j in range(nband)], axis=0
    )
    row_mask = jnp.concatenate([row_mask, row_mask], axis=1)
    col_mask = (rank_next[...] < count).astype(F32)
    col_mask = jnp.concatenate([col_mask, col_mask], axis=1)
    mask = row_mask * col_mask > 0.5

    for c in range(CHUNKS):
        sends[c].wait_recv()
        real, imag = rights[0, chunk(c), :].astype(F32), rights[1, chunk(c), :].astype(F32)
        turn, lift = cosine[chunk(c), :], sine[chunk(c), :]
        new_real = (turn * real + lift * imag).astype(BF16)
        new_imag = (turn * imag - lift * real).astype(BF16)
        paired = jnp.concatenate(
            [
                jnp.concatenate([new_real, new_imag], axis=1),
                jnp.concatenate([new_imag, -new_real], axis=1),
            ],
            axis=0,
        )
        stacked = jnp.concatenate(
            [
                jnp.concatenate([lefts[p, j, chunk(c), :] for j in range(nband)], axis=1)
                for p in range(2)
            ],
            axis=0,
        )
        term = across(stacked, paired, ((0,), (0,)))
        if c == 0:
            acc[...] = term
        elif c < CHUNKS - 1:
            acc[...] += term
        else:
            parts[band, 0] = jnp.where(mask, acc[...] + term, 0.0).astype(BF16)

    def share_sum(d, e, slot):
        block = parts.at[slot, d]
        return remote(
            block, block, sem_sum.at[0, e, d], sem_sum.at[1, e, d],
            {"band": lax.rem(band + e, nband)},
        )

    part_sends = []
    for d in range(1, norb):
        copy = remote(
            parts.at[band, 0], parts.at[band, d], sem_orb.at[0, d], sem_orb.at[1, d],
            {"orb": lax.rem(orb + d, norb)},
        )
        copy.start()
        part_sends.append(copy)
    sum_sends = []
    for d in range(norb):
        if d > 0:
            part_sends[d - 1].wait_recv()
        for e in range(1, nband):
            copy = share_sum(d, e, band)
            copy.start()
            sum_sends.append(copy)
    for d in range(norb):
        for e in range(1, nband):
            share_sum(d, e, lax.rem(band + nband - e, nband)).wait_recv()
    whole = []
    for j in range(nband):
        total = parts[j, 0].astype(F32)
        for d in range(1, norb):
            total += parts[j, d].astype(F32)
        whole.append(total)
    margins = jnp.concatenate(
        [whole[j][:, :cols] for j in range(nband)] + [whole[j][:, cols:] for j in range(nband)],
        axis=1,
    )
    squares = jnp.sum(margins * margins, keepdims=True)
    iterate = margins * (ns_gain * lax.rsqrt(squares / count.astype(F32) + eps_mean))
    for _ in range(NS_STEPS):
        iterate = polar_step(iterate)

    def columns(j):
        at = [iterate[:, p * bands + j * cols : p * bands + (j + 1) * cols] for p in range(2)]
        return jnp.concatenate(at, axis=1)

    mine = columns(0)
    for j in range(1, nband):
        mine = jnp.where(band == j, columns(j), mine)
    cur[...] = mine.astype(BF16)
    share = bands // norb
    my_rows = pl.ds(pl.multiple_of(orb * share, share), share)
    scale = math.sqrt(bands)

    @pl.when(ka == 0)
    def _():
        acc[...] = mine
        out[...] = acc[my_rows, :] * scale
        pfx[...] = cur[my_rows, :]

    for level in range(levels_of(nka) if nka > 1 else 0):
        half = 1 << level
        first = ka < 2 * half
        for is_first in (True, False):
            if not is_first and 2 * half >= nka:
                continue
            height = share if is_first else bands
            source = pfx if is_first else cur
            here = first if is_first else jnp.logical_not(first)
            sending = jnp.logical_and(here, lax.rem(ka, 2 * half) == half - 1)
            taking = jnp.logical_and(here, lax.rem(ka // half, 2) == 1)

            def push(t, level=level, height=height, source=source):
                return remote(
                    source, got.at[level, band, pl.ds(0, height)],
                    sem_pre.at[0, level, t], sem_pre.at[1, level, 0],
                    {"ka": lax.rem(ka + t, nka)},
                )

            def pass_on(d, level=level, height=height):
                block = got.at[level, band, pl.ds(0, height)]
                return remote(
                    block, block, sem_fwd.at[0, level, d], sem_fwd.at[1, level, d],
                    {"band": lax.rem(band + d, nband)},
                )

            for t in range(half, 0, -1):
                @pl.when(jnp.logical_and(sending, ka + t < nka))
                def _(t=t, push=push):
                    push(t).start()

            for t in range(half, 0, -1):
                @pl.when(jnp.logical_and(sending, ka + t < nka))
                def _(t=t, push=push):
                    push(t).wait_send()

            @pl.when(taking)
            def _(level=level, height=height, is_first=is_first, push=push, pass_on=pass_on):
                push(1).wait_recv()
                for d in range(1, nband):
                    pass_on(d).start()
                for d in range(1, nband):
                    came = lax.rem(band + nband - d, nband)
                    block = got.at[level, came, pl.ds(0, height)]
                    remote(
                        block, block, sem_fwd.at[0, level, d], sem_fwd.at[1, level, d],
                        {"band": lax.rem(band + d, nband)},
                    ).wait_recv()
                pieces = [got[level, j, :height, :] for j in range(nband)]
                joined = merge(pieces, cur[...])
                if is_first:
                    out[...] = joined * scale
                    pfx[...] = joined.astype(BF16)
                else:
                    cur[...] = joined.astype(BF16)
                for d in range(1, nband):
                    pass_on(d).wait_send()

    for copy in sends + band_sends + part_sends + sum_sends + [next_rank]:
        copy.wait_send()


def solution(mesh):
    nka, norb, nband = mesh.shape["ka"], mesh.shape["orb"], mesh.shape["band"]
    depth = levels_of(nka)

    def body(eigvecs, band_rank, occ_count, wrap_shift, orbital_site):
        rows, cols = eigvecs.shape[2], eigvecs.shape[3]
        bands = cols * nband
        share = bands // norb
        hbm = pl.BlockSpec(memory_space=pltpu.HBM)
        dma = pltpu.SemaphoreType.DMA
        result = pl.pallas_call(
            functools.partial(kernel, nka, norb, nband),
            out_shape=jax.ShapeDtypeStruct((share, 2 * cols), F32),
            in_specs=[hbm] * 5,
            out_specs=pl.BlockSpec(memory_space=pltpu.VMEM),
            scratch_shapes=[
                pltpu.VMEM((2, nband, rows, cols), BF16),
                pltpu.VMEM((2, rows, cols), BF16),
                pltpu.VMEM((rows, cols), F32),
                pltpu.VMEM((rows, cols), F32),
                pltpu.VMEM((rows // 128, 128), F32),
                pltpu.VMEM((rows // 128, 128), F32),
                pltpu.SMEM((1,), jnp.int32),
                pltpu.SMEM((1,), jnp.int32),
                pltpu.VMEM((rows // 128, 128), jnp.int32),
                pltpu.VMEM((nband, 1, cols), jnp.int32),
                pltpu.VMEM((1, cols), jnp.int32),
                pltpu.VMEM((bands, 2 * cols), F32),
                pltpu.VMEM((nband, norb, bands, 2 * cols), BF16),
                pltpu.VMEM((bands, 2 * cols), BF16),
                pltpu.VMEM((share, 2 * cols), BF16),
                pltpu.VMEM((depth, nband, bands, 2 * cols), BF16),
                dma,
                dma((4,)),
                dma((2, nband)),
                dma((2, nband)),
                dma((2,)),
                dma((2, CHUNKS)),
                dma((2, norb)),
                dma((2, nband, norb)),
                dma((2, depth, max(2, 1 << (depth - 1)) + 1)),
                dma((2, depth, nband)),
            ],
            compiler_params=pltpu.CompilerParams(
                collective_id=0, has_side_effects=True,
                vmem_limit_bytes=67043328
            ),
            name="wilson",
        )(
            eigvecs.reshape(2, rows, cols), band_rank, occ_count, wrap_shift,
            orbital_site.reshape(rows // 128, 128),
        )
        return result.reshape(1, share, 2, cols)

    return jax.shard_map(
        body,
        mesh=mesh,
        in_specs=(
            P(("grp", "ka"), None, "orb", "band"),
            P(("grp", "ka"), "band"),
            P("grp"),
            P("grp"),
            P(("grp", "orb")),
        ),
        out_specs=P(("grp", "ka"), "orb", None, "band"),
        check_vma=False,
    )
```
